512 devices in a mesh: cuts: 4 (over z_hi), fsdp: 128 (over y, x, z_lo, core).
Axes of the slice: x: 4, y: 4, z: 16 (z_hi: 4, z_lo: 4; z = z_hi * 4 + z_lo), core: 2. Of those that a mesh axis runs over, the one named last changes fastest.
Arguments:
- tokens: bfloat16 [65536, 8192], P(('cuts', 'fsdp')), may hold values from -240 to 240
- norm_gain: bfloat16 [8192], P('fsdp'), may hold values from 0.5 to 1.5
- gate_weight: bfloat16 [8192, 256], P('fsdp'), may hold values from -0.0625 to 0.0625
- up_weight: bfloat16 [8192, 256], P('fsdp'), may hold values from -0.0625 to 0.0625
- down_weight: bfloat16 [256, 8192], P(None, 'fsdp'), may hold values from -0.375 to 0.375
- slice_grads: float32 [4, 3, 8192, 256], P('cuts', None, 'fsdp'), may hold values from -6 to 6
Outputs:
- branch_out: bfloat16 [65536, 8192], P(('cuts', 'fsdp'))
- grad_mean: float32 [3, 8192, 256], P(None, 'fsdp')
The draws below stay inside these ranges and needn't reach their ends.
All inputs are finite; a program needn't handle non-finite values.
Results may differ from the reference program's by a relative error of at most 0.0065.
Values may be sent and summed in bfloat16 or wider, within the bound.
No kernel may reach another device: no remote copies, remote signals or barrier semaphores. Data moves between devices by JAX's collectives and lax.ppermute only.
A program may use at most 64 MiB of HBM per device.

```python
import math
import jax
import jax.numpy as jnp
from jax import lax

D = 8192
F = 256
TOK_DEV = 128
TOKENS = 65536
N_CUTS = 4


def draw_tokens(key, part):
    key_base = jax.random.fold_in(key, 11)
    key_rows = jax.random.fold_in(key, 12)
    key_cols = jax.random.fold_in(key, 13)
    base_draw = jax.random.normal(key_base, (TOKENS, D), jnp.float32)
    base_draw = jnp.clip(base_draw, -6.0, 6.0)
    row_scale = jnp.exp(jax.random.uniform(key_rows, (TOKENS, 1), jnp.float32, 0.0, math.log(10.0)))
    col_scale = jnp.exp(jax.random.uniform(key_cols, (1, D), jnp.float32, math.log(0.4), math.log(4.0)))
    return (base_draw * row_scale * col_scale).astype(jnp.bfloat16)


def levels(own_key, extent, cuts, low, high):
    def one(position, blocks):
        draws = jax.random.uniform(jax.random.fold_in(jax.random.fold_in(own_key, 6), position), (blocks,), jnp.float32, low / len(cuts), high / len(cuts))
        return jnp.repeat(jnp.exp(draws), extent[position] // blocks).reshape((-1,) + (1,) * (len(extent) - position - 1))

    loudness = one(*cuts[0])
    for cut in cuts[1:]:
        loudness = loudness * one(*cut)
    return loudness


def gaussian(key, shape, width, most, cuts=(), held_as=jnp.bfloat16):
    loudness = levels(key, shape, cuts, -0.22, 0.18) if cuts else 1.0
    values = jax.random.normal(key, shape, jnp.float32) * width * loudness
    return jnp.minimum(jnp.maximum(values, -most), most).astype(held_as)


def setup_inputs(seed: int = 0) -> dict:
    key_list = jax.random.split(jax.random.key(seed), 7)
    tokens = draw_tokens(jax.random.fold_in(key_list[6], 71), 0)
    norm_gain = jnp.clip(1.0 + 0.1 * jax.random.normal(key_list[1], (D,), jnp.float32), 0.5, 1.5).astype(jnp.bfloat16)
    gate_weight = gaussian(key_list[2], (D, F), D ** -0.5, 0.0625, ((0, 128),))
    up_weight = gaussian(key_list[3], (D, F), D ** -0.5, 0.0625, ((0, 128),))
    down_weight = gaussian(key_list[4], (F, D), F ** -0.5, 0.375, ((1, 128),))
    slice_grads = gaussian(key_list[5], (N_CUTS, 3, D, F), 1.0, 6.0, ((0, 4), (2, 128)), jnp.float32)
    return {"tokens": tokens, "norm_gain": norm_gain, "gate_weight": gate_weight, "up_weight": up_weight, "down_weight": down_weight, "slice_grads": slice_grads}


def feed_block(token_block, norm_gain, gate_weight, up_weight, down_weight):
    tok_float = token_block.astype(jnp.float32)
    inv_rms = lax.rsqrt(lax.optimization_barrier(jnp.mean(tok_float * tok_float, axis=1, keepdims=True)) + 1e-05)
    normed = (tok_float * inv_rms * norm_gain.astype(jnp.float32)[None, :]).astype(jnp.bfloat16)
    gate_out = jnp.dot(normed, gate_weight, preferred_element_type=jnp.float32)
    up_out = jnp.dot(normed, up_weight, preferred_element_type=jnp.float32)
    hidden = (jax.nn.silu(gate_out) * up_out).astype(jnp.bfloat16)
    return jnp.dot(hidden, down_weight, preferred_element_type=jnp.float32).astype(jnp.bfloat16)

def reference(tokens, norm_gain, gate_weight, up_weight, down_weight, slice_grads):
    block_rows = 4 * TOK_DEV
    blocked = tokens.reshape(TOKENS // block_rows, block_rows, D)

    def one_block(token_block):
        return feed_block(token_block, norm_gain, gate_weight, up_weight, down_weight)
    branch_out = lax.map(one_block, blocked).reshape(TOKENS, D)
    grad_mean = lax.optimization_barrier(jnp.sum(slice_grads, axis=0)) / N_CUTS
    return (branch_out, grad_mean)
```

```python
import functools
import itertools

import jax
import jax.numpy as jnp
from jax import lax
from jax.experimental import pallas as pl
from jax.experimental.pallas import tpu as pltpu
from jax.sharding import Mesh
from jax.sharding import PartitionSpec as P

AXES = ("c", "y", "x", "z", "k")
FSDP = AXES[1:]
SUM_DIMS = (((1,), (0,)), ((), ()))
ROW_DIMS = (((1,), (1,)), ((), ()))


def moved(value, sizes, to):
    index = lambda at: functools.reduce(lambda i, s: i * s[1] + s[0], zip(at, sizes), 0)
    pairs = [(index(at), index(to(*at))) for at in itertools.product(*map(range, sizes))]
    return lax.ppermute(value, AXES, pairs)


def over_cuts(m):
    return lambda c, y, x, z, k: (c ^ m, y, x, z, k)


def other_core(c, y, x, z, k):
    return (c, y, x, z, 1 - k)


def first_axis(m):
    return lambda c, y, x, z, k: (c, y ^ (m * k), x ^ (m * (1 - k)), z, k)


def second_axis(m):
    return lambda c, y, x, z, k: (c, y ^ (m * (1 - k)), x ^ (m * k), z, k)


def ffn_kernel(at_ref, inv_ref, tok_ref, *refs):
    own, other, out_ref = refs[:4], refs[4:8], refs[8]
    rows = own[0].shape[1]
    half = own[0].shape[2] // 3
    total = jnp.zeros((tok_ref.shape[0], 4 * half), jnp.float32)
    for a, j in itertools.product(range(4), range(4)):
        start = pl.multiple_of(at_ref[4 * a + j], rows)
        mine = own[a][j, :, : 2 * half]
        theirs = other[j][a, :, : 2 * half]
        both = jnp.concatenate([mine, theirs], axis=1)
        total += lax.dot_general(
            tok_ref[:, pl.ds(start, rows)], both, SUM_DIMS, preferred_element_type=jnp.float32
        )
    total = total * inv_ref[...]
    gate = jnp.concatenate([total[:, :half], total[:, 2 * half : 3 * half]], axis=1)
    up = jnp.concatenate([total[:, half : 2 * half], total[:, 3 * half :]], axis=1)
    hidden = (gate / (1.0 + jnp.exp(-gate)) * up).astype(jnp.bfloat16)
    for a, j in itertools.product(range(4), range(4)):
        start = pl.multiple_of(at_ref[4 * a + j], rows)
        down = jnp.concatenate([own[a][j, :, 2 * half :], other[j][a, :, 2 * half :]], axis=1)
        part = lax.dot_general(hidden, down, ROW_DIMS, preferred_element_type=jnp.float32)
        out_ref[:, pl.ds(start, rows)] = part.astype(out_ref.dtype)


def per_device(sizes, tokens, norm_gain, gate_weight, up_weight, down_weight, slice_grads):
    move = lambda value, to: moved(value, sizes, to)
    y, x, k = lax.axis_index("y"), lax.axis_index("x"), lax.axis_index("k")
    gain = norm_gain.astype(jnp.float32)[:, None]
    gate = (gate_weight.astype(jnp.float32) * gain).astype(jnp.bfloat16)
    up = (up_weight.astype(jnp.float32) * gain).astype(jnp.bfloat16)
    down = down_weight.T
    f = gate.shape[1] // 2
    pack = jnp.concatenate(
        [w[:, s] for s in (slice(0, f), slice(f, 2 * f)) for w in (gate, up, down)], axis=1
    )
    near = lax.all_gather(pack, ("z", "k"), axis=0, tiled=True)
    near = lax.dynamic_slice_in_dim(near, k * 3 * f, 3 * f, axis=1)

    mine = slice_grads[0].astype(jnp.bfloat16)
    near, mine = lax.optimization_barrier((near, mine))
    pair = mine.astype(jnp.float32) + move(mine, over_cuts(1)).astype(jnp.float32)
    pair = pair.astype(jnp.bfloat16)
    line = jnp.stack([near] + [move(near, first_axis(m)) for m in (1, 2, 3)])
    line, pair = lax.optimization_barrier((line, pair))
    own = [line] + [move(line, second_axis(m)) for m in (1, 2, 3)]
    grads = pair.astype(jnp.float32) + move(pair, over_cuts(2)).astype(jnp.float32)
    grad_mean = grads / sizes[0]
    own[1], grad_mean = lax.optimization_barrier((own[1], grad_mean))
    other = [move(a, other_core) for a in own]

    tok_float = tokens.astype(jnp.float32)
    inv_rms = lax.rsqrt(jnp.mean(tok_float * tok_float, axis=1, keepdims=True) + 1e-05)
    a, j = jnp.arange(16) // 4, jnp.arange(16) % 4
    at_y = y ^ jnp.where(k == 0, a, j)
    at_x = x ^ jnp.where(k == 0, j, a)
    at = ((at_y * 4 + at_x) * near.shape[0]).astype(jnp.int32)

    vmem = pl.BlockSpec(memory_space=pltpu.VMEM)
    branch = pl.pallas_call(
        ffn_kernel,
        out_shape=jax.ShapeDtypeStruct(tokens.shape, jnp.bfloat16),
        in_specs=[pl.BlockSpec(memory_space=pltpu.SMEM)] + [vmem] * 10,
        out_specs=vmem,
        name="ffn",
    )(at, inv_rms, tokens, *own, *other)
    return branch, grad_mean


def solution(mesh):
    cuts = mesh.shape["cuts"]
    sizes = (cuts, 4, 4, 4, 2)
    finer = Mesh(mesh.devices.reshape(sizes), AXES)
    in_specs = (
        P(AXES, None),
        P(FSDP),
        P(FSDP, None),
        P(FSDP, None),
        P(None, FSDP),
        P("c", None, FSDP, None),
    )
    out_specs = (P(AXES, None), P(None, FSDP, None))
    return jax.shard_map(
        functools.partial(per_device, sizes),
        mesh=finer,
        in_specs=in_specs,
        out_specs=out_specs,
        check_vma=False,
    )
```

```python
import functools
import itertools

import jax
import jax.numpy as jnp
from jax import lax
from jax.experimental import pallas as pl
from jax.experimental.pallas import tpu as pltpu
from jax.sharding import Mesh
from jax.sharding import PartitionSpec as P

AXES = ("c", "y", "x", "z", "k")
FSDP = AXES[1:]
SUM_DIMS = (((1,), (0,)), ((), ()))
ROW_DIMS = (((1,), (1,)), ((), ()))
VMEM = pl.BlockSpec(memory_space=pltpu.VMEM)
SMEM = pl.BlockSpec(memory_space=pltpu.SMEM)
ANY = pl.BlockSpec(memory_space=pl.ANY)
HBM = pl.BlockSpec(memory_space=pltpu.HBM)
EPS = 1e-05
LANES = 128
SHARE, HALF, WIDE = 512, 256, 256
HALVES = ((0, 1), (3, 2))
EARLY = ((0, 0), (0, 1), (1, 0), (3, 1), (1, 1), (3, 0))
LATE = ((2, 1), (2, 0))
ORDER = EARLY + LATE


def moved(value, sizes, to):
    index = lambda at: functools.reduce(lambda i, s: i * s[1] + s[0], zip(at, sizes), 0)
    pairs = [(index(at), index(to(*at))) for at in itertools.product(*map(range, sizes))]
    return lax.ppermute(value, AXES, pairs)


def over_cuts(m):
    return lambda c, y, x, z, k: (c ^ m, y, x, z, k)


def other_core(c, y, x, z, k):
    return (c, y, x, z, 1 - k)


def first_axis(m):
    return lambda c, y, x, z, k: (c, y ^ (m * k), x ^ (m * (1 - k)), z, k)


def second_axis(m):
    return lambda c, y, x, z, k: (c, y ^ (m * (1 - k)), x ^ (m * k), z, k)


def pack_kernel(gain_hbm, gate_hbm, up_hbm, down_hbm, out_ref, gain_ref, gate_ref, up_ref, sems):
    f = gate_hbm.shape[1]
    copies = [
        pltpu.make_async_copy(a, b, sems.at[n])
        for n, (a, b) in enumerate(
            [
                (gain_hbm, gain_ref),
                (gate_hbm, gate_ref),
                (up_hbm, up_ref),
                (down_hbm, out_ref.at[:, 2 * f :]),
            ]
        )
    ]
    for copy in copies:
        copy.start()
    for copy in copies:
        copy.wait()
    rows = gate_hbm.shape[0]
    at = lambda d: lax.broadcasted_iota(jnp.int32, (rows, rows), d)
    gain = jnp.where(at(0) == at(1), gain_ref[...].astype(jnp.float32), 0.0)
    gain = jnp.sum(gain, axis=1, keepdims=True)
    gate = (gate_ref[...].astype(jnp.float32) * gain).astype(out_ref.dtype)
    up = (up_ref[...].astype(jnp.float32) * gain).astype(out_ref.dtype)
    h = f // 2
    for k in range(2):
        for n, w in enumerate((gate, up)):
            out_ref[:, (2 * k + n) * h : (2 * k + n + 1) * h] = w[:, k * h : (k + 1) * h]


def pack(gain, gate, up, down):
    rows, f = gate.shape
    return pl.pallas_call(
        pack_kernel,
        out_shape=jax.ShapeDtypeStruct((rows, 3 * f), gate.dtype),
        in_specs=[ANY] * 4,
        out_specs=VMEM,
        scratch_shapes=[
            pltpu.VMEM((1, rows), gate.dtype),
            pltpu.VMEM((rows, f), gate.dtype),
            pltpu.VMEM((rows, f), gate.dtype),
            pltpu.SemaphoreType.DMA((4,)),
        ],
        name="pack",
    )(gain[None, :], gate, up, down)


def load_tokens(steps, at_ref, toks, tok_ref, sems):
    rows = toks[0].shape[0]
    copies = []
    for s, (a, half) in enumerate(steps):
        for i, j in enumerate(HALVES[half]):
            start = pl.multiple_of(at_ref[4 * a + j], SHARE)
            for who in range(2):
                copies.append(
                    pltpu.make_async_copy(
                        toks[who].at[:, pl.ds(start, SHARE)],
                        tok_ref.at[s, i, who * rows : (who + 1) * rows, :],
                        sems.at[s, i, who],
                    )
                )
    for copy in copies:
        copy.start()
    return copies


def add_piece(total, square, tok, gate_up):
    total += lax.dot_general(tok, gate_up, SUM_DIMS, preferred_element_type=jnp.float32)
    for l in range(0, SHARE, LANES):
        t = tok[:, l : l + LANES].astype(jnp.float32)
        square += t * t
    return total, square


def early_kernel(at_ref, *refs):
    n = len(EARLY)
    toks, pieces, (out_ref, down_ref, tok_ref, sems) = refs[:2], refs[2 : 2 + n], refs[2 + n :]
    copies = load_tokens(EARLY, at_ref, toks, tok_ref, sems)
    for s in range(n):
        down_ref[s] = pieces[s][:, SHARE:, :]
    total = jnp.zeros((2 * toks[0].shape[0], WIDE), jnp.float32)
    square = jnp.zeros((2 * toks[0].shape[0], LANES), jnp.float32)
    for s, i in itertools.product(range(n), range(2)):
        for who in range(2):
            copies[4 * s + 2 * i + who].wait()
        total, square = add_piece(total, square, tok_ref[s, i], pieces[s][i, :SHARE, :])
    out_ref[:, :WIDE] = total
    out_ref[:, WIDE:] = square


def late_kernel(at_ref, before_ref, *refs):
    n = len(LATE)
    toks, pieces, (mine_ref, send_ref, tok_ref, sems) = refs[:2], refs[2 : 2 + n], refs[2 + n :]
    rows = toks[0].shape[0]
    copies = load_tokens(LATE, at_ref, toks, tok_ref, sems)
    for part, (s, i) in enumerate(itertools.product(range(n), range(2))):
        send_ref[part * HALF : (part + 1) * HALF, :] = pieces[s][i, SHARE:, :]
    total, square = before_ref[:, :WIDE], before_ref[:, WIDE:]
    for s, i in itertools.product(range(n), range(2)):
        for who in range(2):
            copies[4 * s + 2 * i + who].wait()
        total, square = add_piece(total, square, tok_ref[s, i], pieces[s][i, :SHARE, :])
    mean = jnp.sum(square, axis=1, keepdims=True) / (2 * len(ORDER) * SHARE)
    total = total * lax.rsqrt(mean + EPS)
    gate, up = total[:, : WIDE // 2], total[:, WIDE // 2 :]
    hidden = (gate / (1.0 + jnp.exp(-gate)) * up).astype(jnp.bfloat16)
    mine_ref[...] = hidden[:rows]
    send_ref[2 * n * HALF :, : WIDE // 2] = hidden[rows:]
    send_ref[2 * n * HALF :, WIDE // 2 :] = hidden[:rows]


def sums_params(n):
    return dict(
        compiler_params=pltpu.CompilerParams(vmem_limit_bytes=8 * 2**20),
        cost_estimate=pl.CostEstimate(flops=n * 2**30, bytes_accessed=n * 2**20, transcendentals=0),
    )


def token_scratch(n, rows):
    return [
        pltpu.VMEM((n, 2, 2 * rows, SHARE), jnp.bfloat16),
        pltpu.SemaphoreType.DMA((n, 2, 2)),
    ]


def early_sums(at, tokens, pieces):
    n, rows = len(EARLY), tokens[0].shape[0]
    return pl.pallas_call(
        early_kernel,
        out_shape=[
            jax.ShapeDtypeStruct((2 * rows, WIDE + LANES), jnp.float32),
            jax.ShapeDtypeStruct((n, 2, HALF, WIDE), jnp.bfloat16),
        ],
        in_specs=[SMEM] + [HBM] * 2 + [VMEM] * n,
        out_specs=[VMEM, VMEM],
        scratch_shapes=token_scratch(n, rows),
        name="early",
        **sums_params(n),
    )(at, *tokens, *[pieces[s] for s in EARLY])


def late_sums(at, before, tokens, pieces):
    n, rows = len(LATE), tokens[0].shape[0]
    return pl.pallas_call(
        late_kernel,
        out_shape=[
            jax.ShapeDtypeStruct((rows, WIDE // 2), jnp.bfloat16),
            jax.ShapeDtypeStruct((2 * n * HALF + rows, WIDE), jnp.bfloat16),
        ],
        in_specs=[SMEM, VMEM] + [HBM] * 2 + [VMEM] * n,
        out_specs=[VMEM, VMEM],
        scratch_shapes=token_scratch(n, rows),
        name="late",
        **sums_params(n),
    )(at, before, *tokens, *[pieces[s] for s in LATE])


def down_kernel(at_ref, mine_ref, early_ref, late_ref, *refs):
    n = len(ORDER)
    own, (out_ref, out_held, out_sems) = refs[:n], refs[n:]
    mine, theirs = mine_ref[...], late_ref[2 * len(LATE) * HALF :, : WIDE // 2]
    hidden = jnp.where(
        at_ref[48] == 0,
        jnp.concatenate([mine, theirs], axis=1),
        jnp.concatenate([theirs, mine], axis=1),
    )
    copies = []
    for slot, (s, i, who) in enumerate(itertools.product(range(n), range(2), range(2))):
        a, half = ORDER[s]
        if who == 0:
            rows = own[s][i, SHARE:, :]
        elif s < len(EARLY):
            rows = early_ref[s, i]
        else:
            part = 2 * (s - len(EARLY)) + i
            rows = late_ref[part * HALF : (part + 1) * HALF, :]
        out = lax.dot_general(hidden, rows, ROW_DIMS, preferred_element_type=jnp.float32)
        out_held[slot] = out.astype(out_held.dtype)
        start = pl.multiple_of(at_ref[16 + 16 * who + 4 * a + HALVES[half][i]], HALF)
        copy = pltpu.make_async_copy(
            out_held.at[slot], out_ref.at[:, pl.ds(start, HALF)], out_sems.at[slot]
        )
        copy.start()
        copies.append(copy)
    for copy in copies:
        copy.wait()


def down(at, mine, early, late, own, tokens):
    n = len(ORDER)
    rows = tokens.shape[0]
    return pl.pallas_call(
        down_kernel,
        out_shape=jax.ShapeDtypeStruct(tokens.shape, jnp.bfloat16),
        in_specs=[SMEM] + [VMEM] * (n + 3),
        out_specs=HBM,
        scratch_shapes=[
            pltpu.VMEM((4 * n, rows, HALF), jnp.bfloat16),
            pltpu.SemaphoreType.DMA((4 * n,)),
        ],
        compiler_params=pltpu.CompilerParams(vmem_limit_bytes=8 * 2**20),
        name="down",
    )(at, mine, early, late, *[own[s] for s in ORDER])


def per_device(sizes, tokens, norm_gain, gate_weight, up_weight, down_weight, slice_grads):
    move = lambda value, to: moved(value, sizes, to)
    y, x, k = lax.axis_index("y"), lax.axis_index("x"), lax.axis_index("k")
    packed = pack(norm_gain, gate_weight, up_weight, down_weight.T)
    near = lax.all_gather(packed, ("z", "k"), axis=0, tiled=True)
    near = jnp.concatenate(
        [
            lax.dynamic_slice(near, (0, k * WIDE), (SHARE, WIDE)),
            lax.dynamic_slice(near, (k * HALF, 2 * WIDE), (HALF, WIDE)),
        ]
    )
    near, grads = lax.optimization_barrier((near, slice_grads[0]))
    mine = grads.astype(jnp.bfloat16)
    line = {m: move(near, first_axis(m)) for m in (1, 3, 2)}
    line[0] = near
    far = move(mine, over_cuts(1))
    both_tokens = (tokens, move(tokens, other_core))

    own = {}
    for h in range(2):
        own[0, h] = jnp.stack([line[j] for j in HALVES[h]])
    own[1, 0] = move(own[0, 0], second_axis(1))
    own[3, 1] = move(own[0, 1], second_axis(3))
    own[1, 1] = move(own[0, 1], second_axis(1))
    own[3, 0] = move(own[0, 0], second_axis(3))
    own[2, 0] = move(own[1, 0], second_axis(3))
    own[2, 1] = move(own[3, 1], second_axis(1))

    a, j = jnp.arange(16) // 4, jnp.arange(16) % 4
    place = lambda core: (y ^ jnp.where(core == 0, a, j)) * 4 + (x ^ jnp.where(core == 0, j, a))
    at = jnp.concatenate(
        [
            place(k) * SHARE,
            place(k) * SHARE + k * HALF,
            place(1 - k) * SHARE + (1 - k) * HALF,
            k[None],
        ]
    ).astype(jnp.int32)

    total, early = early_sums(at, both_tokens, own)
    early = move(early, other_core)
    pair = (mine.astype(jnp.float32) + far.astype(jnp.float32)).astype(jnp.bfloat16)
    rest = move(pair, over_cuts(3))
    grad_mean = (pair.astype(jnp.float32) + rest.astype(jnp.float32)) / sizes[0]
    mine_hidden, late = late_sums(at, total, both_tokens, own)
    late = move(late, other_core)
    branch = down(at, mine_hidden, early, late, own, tokens)
    return branch, grad_mean


def solution(mesh):
    cuts = mesh.shape["cuts"]
    sizes = (cuts, 4, 4, 4, 2)
    finer = Mesh(mesh.devices.reshape(sizes), AXES)
    in_specs = (
        P(AXES, None),
        P(FSDP),
        P(FSDP, None),
        P(FSDP, None),
        P(None, FSDP),
        P("c", None, FSDP, None),
    )
    out_specs = (P(AXES, None), P(None, FSDP, None))

    def body(*args):
        return per_device(sizes, *args)

    return jax.shard_map(
        body, mesh=finer, in_specs=in_specs, out_specs=out_specs, check_vma=False
    )
```

```python
import functools
import itertools

import jax
import jax.numpy as jnp
from jax import lax
from jax.experimental import pallas as pl
from jax.experimental.pallas import tpu as pltpu
from jax.sharding import Mesh
from jax.sharding import PartitionSpec as P

AXES = ("c", "y", "x", "z", "k")
FSDP = AXES[1:]
SUM_DIMS = (((1,), (0,)), ((), ()))
ROW_DIMS = (((1,), (1,)), ((), ()))
VMEM = pl.BlockSpec(memory_space=pltpu.VMEM)
SMEM = pl.BlockSpec(memory_space=pltpu.SMEM)
ANY = pl.BlockSpec(memory_space=pl.ANY)
HBM = pl.BlockSpec(memory_space=pltpu.HBM)
EPS = 1e-05
LANES = 128
SHARE, HALF, WIDE = 512, 256, 256
HALVES = ((0, 1), (3, 2))
EARLY = ((0, 0), (0, 1), (1, 0), (3, 1), (1, 1), (3, 0))
LATE = ((2, 1), (2, 0))
ORDER = EARLY + LATE


def moved(value, sizes, to):
    index = lambda at: functools.reduce(lambda i, s: i * s[1] + s[0], zip(at, sizes), 0)
    pairs = [(index(at), index(to(*at))) for at in itertools.product(*map(range, sizes))]
    return lax.ppermute(value, AXES, pairs)


def over_cuts(m):
    return lambda c, y, x, z, k: (c ^ m, y, x, z, k)


def other_core(c, y, x, z, k):
    return (c, y, x, z, 1 - k)


def first_axis(m):
    return lambda c, y, x, z, k: (c, y ^ (m * k), x ^ (m * (1 - k)), z, k)


def second_axis(m):
    return lambda c, y, x, z, k: (c, y ^ (m * (1 - k)), x ^ (m * k), z, k)


def pack_kernel(gain_hbm, gate_hbm, up_hbm, down_hbm, out_ref, gain_ref, gate_ref, up_ref, sems):
    f = gate_hbm.shape[1]
    copies = [
        pltpu.make_async_copy(a, b, sems.at[n])
        for n, (a, b) in enumerate(
            [
                (gain_hbm, gain_ref),
                (gate_hbm, gate_ref),
                (up_hbm, up_ref),
                (down_hbm, out_ref.at[:, 2 * f :]),
            ]
        )
    ]
    for copy in copies:
        copy.start()
    for copy in copies:
        copy.wait()
    rows = gate_hbm.shape[0]
    at = lambda d: lax.broadcasted_iota(jnp.int32, (rows, rows), d)
    gain = jnp.where(at(0) == at(1), gain_ref[...].astype(jnp.float32), 0.0)
    gain = jnp.sum(gain, axis=1, keepdims=True)
    gate = (gate_ref[...].astype(jnp.float32) * gain).astype(out_ref.dtype)
    up = (up_ref[...].astype(jnp.float32) * gain).astype(out_ref.dtype)
    h = f // 2
    for k in range(2):
        for n, w in enumerate((gate, up)):
            out_ref[:, (2 * k + n) * h : (2 * k + n + 1) * h] = w[:, k * h : (k + 1) * h]


def pack(gain, gate, up, down):
    rows, f = gate.shape
    return pl.pallas_call(
        pack_kernel,
        out_shape=jax.ShapeDtypeStruct((rows, 3 * f), gate.dtype),
        in_specs=[ANY] * 4,
        out_specs=VMEM,
        scratch_shapes=[
            pltpu.VMEM((1, rows), gate.dtype),
            pltpu.VMEM((rows, f), gate.dtype),
            pltpu.VMEM((rows, f), gate.dtype),
            pltpu.SemaphoreType.DMA((4,)),
        ],
        name="pack",
    )(gain[None, :], gate, up, down)


def token_copies(steps, at_ref, toks, tok_ref, sems):
    rows = toks[0].shape[0]
    copies = []
    for s, (a, half) in enumerate(steps):
        for i, j in enumerate(HALVES[half]):
            start = pl.multiple_of(at_ref[4 * a + j], SHARE)
            for who in range(2):
                copies.append(
                    pltpu.make_async_copy(
                        toks[who].at[:, pl.ds(start, SHARE)],
                        tok_ref.at[s, i, who * rows : (who + 1) * rows, :],
                        sems.at[s, i, who],
                    )
                )
    return copies


def add_piece(total, square, tok, gate_up):
    total += lax.dot_general(tok, gate_up, SUM_DIMS, preferred_element_type=jnp.float32)
    for l in range(0, SHARE, LANES):
        t = tok[:, l : l + LANES].astype(jnp.float32)
        square += t * t
    return total, square


def early_kernel(at_ref, *refs):
    n = len(EARLY)
    toks, pieces = refs[:2], refs[2 : 2 + n]
    out_ref, down_ref, late_tok_ref, tok_ref, sems, late_sems = refs[2 + n :]
    copies = token_copies(EARLY, at_ref, toks, tok_ref, sems)
    late_copies = token_copies(LATE, at_ref, toks, late_tok_ref, late_sems)
    for copy in copies + late_copies:
        copy.start()
    for s in range(n):
        down_ref[s] = pieces[s][:, SHARE:, :]
    total = jnp.zeros((2 * toks[0].shape[0], WIDE), jnp.float32)
    square = jnp.zeros((2 * toks[0].shape[0], LANES), jnp.float32)
    for s, i in itertools.product(range(n), range(2)):
        for who in range(2):
            copies[4 * s + 2 * i + who].wait()
        total, square = add_piece(total, square, tok_ref[s, i], pieces[s][i, :SHARE, :])
    out_ref[:, :WIDE] = total
    out_ref[:, WIDE:] = square
    for copy in late_copies:
        copy.wait()


def late_kernel(before_ref, tok_ref, *refs):
    n = len(LATE)
    pieces, (mine_ref, send_ref) = refs[:n], refs[n:]
    rows = mine_ref.shape[0]
    for part, (s, i) in enumerate(itertools.product(range(n), range(2))):
        send_ref[part * HALF : (part + 1) * HALF, :] = pieces[s][i, SHARE:, :]
    total, square = before_ref[:, :WIDE], before_ref[:, WIDE:]
    for s, i in itertools.product(range(n), range(2)):
        total, square = add_piece(total, square, tok_ref[s, i], pieces[s][i, :SHARE, :])
    mean = jnp.sum(square, axis=1, keepdims=True) / (2 * len(ORDER) * SHARE)
    total = total * lax.rsqrt(mean + EPS)
    gate, up = total[:, : WIDE // 2], total[:, WIDE // 2 :]
    hidden = (gate / (1.0 + jnp.exp(-gate)) * up).astype(jnp.bfloat16)
    mine_ref[...] = hidden[:rows]
    send_ref[2 * n * HALF :, : WIDE // 2] = hidden[rows:]
    send_ref[2 * n * HALF :, WIDE // 2 :] = hidden[:rows]


def sums_params(n):
    return dict(
        compiler_params=pltpu.CompilerParams(vmem_limit_bytes=8 * 2**20),
        cost_estimate=pl.CostEstimate(flops=n * 2**30, bytes_accessed=n * 2**20, transcendentals=0),
    )


def early_sums(at, tokens, pieces):
    n, m, rows = len(EARLY), len(LATE), tokens[0].shape[0]
    return pl.pallas_call(
        early_kernel,
        out_shape=[
            jax.ShapeDtypeStruct((2 * rows, WIDE + LANES), jnp.float32),
            jax.ShapeDtypeStruct((n, 2, HALF, WIDE), jnp.bfloat16),
            jax.ShapeDtypeStruct((m, 2, 2 * rows, SHARE), jnp.bfloat16),
        ],
        in_specs=[SMEM] + [HBM] * 2 + [VMEM] * n,
        out_specs=[VMEM, VMEM, VMEM],
        scratch_shapes=[
            pltpu.VMEM((n, 2, 2 * rows, SHARE), jnp.bfloat16),
            pltpu.SemaphoreType.DMA((n, 2, 2)),
            pltpu.SemaphoreType.DMA((m, 2, 2)),
        ],
        name="early",
        **sums_params(n),
    )(at, *tokens, *[pieces[s] for s in EARLY])


def late_sums(before, late_tokens, rows, pieces):
    n = len(LATE)
    return pl.pallas_call(
        late_kernel,
        out_shape=[
            jax.ShapeDtypeStruct((rows, WIDE // 2), jnp.bfloat16),
            jax.ShapeDtypeStruct((2 * n * HALF + rows, WIDE), jnp.bfloat16),
        ],
        in_specs=[VMEM] * (2 + n),
        out_specs=[VMEM, VMEM],
        name="late",
        **sums_params(n),
    )(before, late_tokens, *[pieces[s] for s in LATE])


def down_kernel(at_ref, mine_ref, early_ref, late_ref, *refs):
    n = len(ORDER)
    own, (out_ref, out_held, out_sems) = refs[:n], refs[n:]
    mine, theirs = mine_ref[...], late_ref[2 * len(LATE) * HALF :, : WIDE // 2]
    hidden = jnp.where(
        at_ref[48] == 0,
        jnp.concatenate([mine, theirs], axis=1),
        jnp.concatenate([theirs, mine], axis=1),
    )
    copies = []
    for slot, (s, i, who) in enumerate(itertools.product(range(n), range(2), range(2))):
        a, half = ORDER[s]
        if who == 0:
            rows = own[s][i, SHARE:, :]
        elif s < len(EARLY):
            rows = early_ref[s, i]
        else:
            part = 2 * (s - len(EARLY)) + i
            rows = late_ref[part * HALF : (part + 1) * HALF, :]
        out = lax.dot_general(hidden, rows, ROW_DIMS, preferred_element_type=jnp.float32)
        out_held[slot] = out.astype(out_held.dtype)
        start = pl.multiple_of(at_ref[16 + 16 * who + 4 * a + HALVES[half][i]], HALF)
        copy = pltpu.make_async_copy(
            out_held.at[slot], out_ref.at[:, pl.ds(start, HALF)], out_sems.at[slot]
        )
        copy.start()
        copies.append(copy)
    for copy in copies:
        copy.wait()


def down(at, mine, early, late, own, tokens):
    n = len(ORDER)
    rows = tokens.shape[0]
    return pl.pallas_call(
        down_kernel,
        out_shape=jax.ShapeDtypeStruct(tokens.shape, jnp.bfloat16),
        in_specs=[SMEM] + [VMEM] * (n + 3),
        out_specs=HBM,
        scratch_shapes=[
            pltpu.VMEM((4 * n, rows, HALF), jnp.bfloat16),
            pltpu.SemaphoreType.DMA((4 * n,)),
        ],
        compiler_params=pltpu.CompilerParams(vmem_limit_bytes=8 * 2**20),
        name="down",
    )(at, mine, early, late, *[own[s] for s in ORDER])


def per_device(sizes, tokens, norm_gain, gate_weight, up_weight, down_weight, slice_grads):
    move = lambda value, to: moved(value, sizes, to)
    y, x, k = lax.axis_index("y"), lax.axis_index("x"), lax.axis_index("k")
    packed = pack(norm_gain, gate_weight, up_weight, down_weight.T)
    near = lax.all_gather(packed, ("z", "k"), axis=0, tiled=True)
    near = jnp.concatenate(
        [
            lax.dynamic_slice(near, (0, k * WIDE), (SHARE, WIDE)),
            lax.dynamic_slice(near, (k * HALF, 2 * WIDE), (HALF, WIDE)),
        ]
    )
    near, grads = lax.optimization_barrier((near, slice_grads[0]))
    mine = grads.astype(jnp.bfloat16)
    line = {m: move(near, first_axis(m)) for m in (1, 3, 2)}
    line[0] = near
    far = move(mine, over_cuts(1))
    both_tokens = (tokens, move(tokens, other_core))

    own = {}
    for h in range(2):
        own[0, h] = jnp.stack([line[j] for j in HALVES[h]])
    own[1, 0] = move(own[0, 0], second_axis(1))
    own[3, 1] = move(own[0, 1], second_axis(3))
    own[1, 1] = move(own[0, 1], second_axis(1))
    own[3, 0] = move(own[0, 0], second_axis(3))
    own[2, 0] = move(own[1, 0], second_axis(3))
    own[2, 1] = move(own[3, 1], second_axis(1))

    a, j = jnp.arange(16) // 4, jnp.arange(16) % 4
    place = lambda core: (y ^ jnp.where(core == 0, a, j)) * 4 + (x ^ jnp.where(core == 0, j, a))
    at = jnp.concatenate(
        [
            place(k) * SHARE,
            place(k) * SHARE + k * HALF,
            place(1 - k) * SHARE + (1 - k) * HALF,
            k[None],
        ]
    ).astype(jnp.int32)

    total, early, late_tokens = early_sums(at, both_tokens, own)
    early = move(early, other_core)
    pair = (mine.astype(jnp.float32) + far.astype(jnp.float32)).astype(jnp.bfloat16)
    rest = move(pair, over_cuts(3))
    grad_mean = (pair.astype(jnp.float32) + rest.astype(jnp.float32)) / sizes[0]
    mine_hidden, late = late_sums(total, late_tokens, tokens.shape[0], own)
    late = move(late, other_core)
    branch = down(at, mine_hidden, early, late, own, tokens)
    return branch, grad_mean


def solution(mesh):
    cuts = mesh.shape["cuts"]
    sizes = (cuts, 4, 4, 4, 2)
    finer = Mesh(mesh.devices.reshape(sizes), AXES)
    in_specs = (
        P(AXES, None),
        P(FSDP),
        P(FSDP, None),
        P(FSDP, None),
        P(None, FSDP),
        P("c", None, FSDP, None),
    )
    out_specs = (P(AXES, None), P(None, FSDP, None))

    def body(*args):
        return per_device(sizes, *args)

    return jax.shard_map(
        body, mesh=finer, in_specs=in_specs, out_specs=out_specs, check_vma=False
    )
```

```python
import functools
import itertools

import jax
import jax.numpy as jnp
from jax import lax
from jax.experimental import pallas as pl
from jax.experimental.pallas import tpu as pltpu
from jax.sharding import Mesh
from jax.sharding import PartitionSpec as P

AXES = ("c", "y", "x", "z", "k")
FSDP = AXES[1:]
SUM_DIMS = (((1,), (0,)), ((), ()))
ROW_DIMS = (((1,), (1,)), ((), ()))
VMEM = pl.BlockSpec(memory_space=pltpu.VMEM)
SMEM = pl.BlockSpec(memory_space=pltpu.SMEM)
ANY = pl.BlockSpec(memory_space=pl.ANY)
HBM = pl.BlockSpec(memory_space=pltpu.HBM)
EPS = 1e-05
LANES = 128
SHARE, HALF, WIDE = 512, 256, 256
HALVES = ((0, 1), (3, 2))
EARLY = ((0, 0), (0, 1), (1, 0), (3, 1), (1, 1), (3, 0))
LATE = ((2, 1), (2, 0))
ORDER = EARLY + LATE


def moved(value, sizes, to):
    index = lambda at: functools.reduce(lambda i, s: i * s[1] + s[0], zip(at, sizes), 0)
    pairs = [(index(at), index(to(*at))) for at in itertools.product(*map(range, sizes))]
    return lax.ppermute(value, AXES, pairs)


def over_cuts(m):
    return lambda c, y, x, z, k: (c ^ m, y, x, z, k)


def other_core(c, y, x, z, k):
    return (c, y, x, z, 1 - k)


def first_axis(m):
    return lambda c, y, x, z, k: (c, y ^ (m * k), x ^ (m * (1 - k)), z, k)


def second_axis(m):
    return lambda c, y, x, z, k: (c, y ^ (m * (1 - k)), x ^ (m * k), z, k)


def pack_kernel(gain_hbm, gate_hbm, up_hbm, down_hbm, out_ref, gain_ref, gate_ref, up_ref, sems):
    f = gate_hbm.shape[1]
    copies = [
        pltpu.make_async_copy(a, b, sems.at[n])
        for n, (a, b) in enumerate(
            [
                (gain_hbm, gain_ref),
                (gate_hbm, gate_ref),
                (up_hbm, up_ref),
                (down_hbm, out_ref.at[:, 2 * f :]),
            ]
        )
    ]
    for copy in copies:
        copy.start()
    for copy in copies:
        copy.wait()
    rows = gate_hbm.shape[0]
    at = lambda d: lax.broadcasted_iota(jnp.int32, (rows, rows), d)
    gain = jnp.where(at(0) == at(1), gain_ref[...].astype(jnp.float32), 0.0)
    gain = jnp.sum(gain, axis=1, keepdims=True)
    gate = (gate_ref[...].astype(jnp.float32) * gain).astype(out_ref.dtype)
    up = (up_ref[...].astype(jnp.float32) * gain).astype(out_ref.dtype)
    h = f // 2
    for k in range(2):
        for n, w in enumerate((gate, up)):
            out_ref[:, (2 * k + n) * h : (2 * k + n + 1) * h] = w[:, k * h : (k + 1) * h]


def pack(gain, gate, up, down):
    rows, f = gate.shape
    return pl.pallas_call(
        pack_kernel,
        out_shape=jax.ShapeDtypeStruct((rows, 3 * f), gate.dtype),
        in_specs=[ANY] * 4,
        out_specs=VMEM,
        scratch_shapes=[
            pltpu.VMEM((1, rows), gate.dtype),
            pltpu.VMEM((rows, f), gate.dtype),
            pltpu.VMEM((rows, f), gate.dtype),
            pltpu.SemaphoreType.DMA((4,)),
        ],
        name="pack",
    )(gain[None, :], gate, up, down)


def token_copies(steps, at_ref, toks, tok_ref, sems):
    rows = toks[0].shape[0]
    copies = []
    for s, (a, half) in enumerate(steps):
        for i, j in enumerate(HALVES[half]):
            start = pl.multiple_of(at_ref[4 * a + j], SHARE)
            for who in range(2):
                copies.append(
                    pltpu.make_async_copy(
                        toks[who].at[:, pl.ds(start, SHARE)],
                        tok_ref.at[s, i, who * rows : (who + 1) * rows, :],
                        sems.at[s, i, who],
                    )
                )
    return copies


def add_piece(total, square, tok, gate_up):
    total += lax.dot_general(tok, gate_up, SUM_DIMS, preferred_element_type=jnp.float32)
    for l in range(0, SHARE, LANES):
        t = tok[:, l : l + LANES].astype(jnp.float32)
        square += t * t
    return total, square


def early_kernel(at_ref, *refs):
    n = len(EARLY)
    toks, pieces = refs[:2], list(refs[2 : 2 + n])
    out_ref, down_ref, late_tok_ref, tok_ref, held, sems, late_sems, held_sems = refs[2 + n :]
    loads = {}
    for i in range(held.shape[0]):
        s = n - held.shape[0] + i
        loads[s] = pltpu.make_async_copy(pieces[s], held.at[i], held_sems.at[i])
        pieces[s] = held.at[i]
    copies = token_copies(EARLY, at_ref, toks, tok_ref, sems)
    late_copies = token_copies(LATE, at_ref, toks, late_tok_ref, late_sems)
    for copy in copies[:8] + list(loads.values()) + copies[8:] + late_copies:
        copy.start()
    total = jnp.zeros((2 * toks[0].shape[0], WIDE), jnp.float32)
    square = jnp.zeros((2 * toks[0].shape[0], LANES), jnp.float32)
    for s in range(n):
        if s in loads:
            loads[s].wait()
        down_ref[s] = pieces[s][:, SHARE:, :]
        for i in range(2):
            for who in range(2):
                copies[4 * s + 2 * i + who].wait()
            total, square = add_piece(total, square, tok_ref[s, i], pieces[s][i, :SHARE, :])
    out_ref[:, :WIDE] = total
    out_ref[:, WIDE:] = square
    for copy in late_copies:
        copy.wait()


def late_kernel(before_ref, tok_ref, *refs):
    n = len(LATE)
    pieces, send_ref = refs[:n], refs[n]
    rows = tok_ref.shape[2] // 2
    for part, (s, i) in enumerate(itertools.product(range(n), range(2))):
        send_ref[part * HALF : (part + 1) * HALF, :] = pieces[s][i, SHARE:, :]
    total, square = before_ref[:, :WIDE], before_ref[:, WIDE:]
    for s, i in itertools.product(range(n), range(2)):
        total, square = add_piece(total, square, tok_ref[s, i], pieces[s][i, :SHARE, :])
    mean = jnp.sum(square, axis=1, keepdims=True) / (2 * len(ORDER) * SHARE)
    total = total * lax.rsqrt(mean + EPS)
    gate, up = total[:, : WIDE // 2], total[:, WIDE // 2 :]
    hidden = (gate / (1.0 + jnp.exp(-gate)) * up).astype(jnp.bfloat16)
    send_ref[2 * n * HALF :, : WIDE // 2] = hidden[rows:]
    send_ref[2 * n * HALF :, WIDE // 2 :] = hidden[:rows]


def sums_params(n):
    return dict(
        compiler_params=pltpu.CompilerParams(vmem_limit_bytes=8 * 2**20),
        cost_estimate=pl.CostEstimate(flops=n * 2**30, bytes_accessed=n * 2**20, transcendentals=0),
    )


def early_sums(at, tokens, pieces):
    n, m, rows = len(EARLY), len(LATE), tokens[0].shape[0]
    return pl.pallas_call(
        early_kernel,
        out_shape=[
            jax.ShapeDtypeStruct((2 * rows, WIDE + LANES), jnp.float32),
            jax.ShapeDtypeStruct((n, 2, HALF, WIDE), jnp.bfloat16),
            jax.ShapeDtypeStruct((m, 2, 2 * rows, SHARE), jnp.bfloat16),
        ],
        in_specs=[SMEM] + [HBM] * 2 + [VMEM] * (n - 2) + [HBM] * 2,
        out_specs=[VMEM, VMEM, VMEM],
        scratch_shapes=[
            pltpu.VMEM((n, 2, 2 * rows, SHARE), jnp.bfloat16),
            pltpu.VMEM((2, 2, SHARE + HALF, WIDE), jnp.bfloat16),
            pltpu.SemaphoreType.DMA((n, 2, 2)),
            pltpu.SemaphoreType.DMA((m, 2, 2)),
            pltpu.SemaphoreType.DMA((2,)),
        ],
        name="early",
        **sums_params(n),
    )(at, *tokens, *[pieces[s] for s in EARLY])


def late_sums(before, late_tokens, rows, pieces):
    n = len(LATE)
    return pl.pallas_call(
        late_kernel,
        out_shape=jax.ShapeDtypeStruct((2 * n * HALF + rows, WIDE), jnp.bfloat16),
        in_specs=[VMEM] * (2 + n),
        out_specs=VMEM,
        name="late",
        **sums_params(n),
    )(before, late_tokens, *[pieces[s] for s in LATE])


def down_kernel(at_ref, own_early_ref, own_late_ref, early_ref, late_ref, out_ref, held, sems):
    half = WIDE // 2
    hid = 2 * len(LATE) * HALF
    mine, theirs = own_late_ref[hid:, half:], late_ref[hid:, :half]
    hidden = jnp.where(
        at_ref[48] == 0,
        jnp.concatenate([mine, theirs], axis=1),
        jnp.concatenate([theirs, mine], axis=1),
    )
    copies = []
    for slot, (s, i, who) in enumerate(itertools.product(range(len(ORDER)), range(2), range(2))):
        a, which = ORDER[s]
        if s < len(EARLY):
            rows = (own_early_ref, early_ref)[who][s, i]
        else:
            part = 2 * (s - len(EARLY)) + i
            rows = (own_late_ref, late_ref)[who][part * HALF : (part + 1) * HALF, :]
        out = lax.dot_general(hidden, rows, ROW_DIMS, preferred_element_type=jnp.float32)
        held[slot] = out.astype(held.dtype)
        start = pl.multiple_of(at_ref[16 + 16 * who + 4 * a + HALVES[which][i]], HALF)
        copy = pltpu.make_async_copy(held.at[slot], out_ref.at[:, pl.ds(start, HALF)], sems.at[slot])
        copy.start()
        copies.append(copy)
    for copy in copies:
        copy.wait()


def down(at, own_early, own_late, early, late, tokens):
    n = len(ORDER)
    return pl.pallas_call(
        down_kernel,
        out_shape=jax.ShapeDtypeStruct(tokens.shape, jnp.bfloat16),
        in_specs=[SMEM] + [VMEM] * 4,
        out_specs=HBM,
        scratch_shapes=[
            pltpu.VMEM((4 * n, tokens.shape[0], HALF), jnp.bfloat16),
            pltpu.SemaphoreType.DMA((4 * n,)),
        ],
        compiler_params=pltpu.CompilerParams(vmem_limit_bytes=8 * 2**20),
        name="down",
    )(at, own_early, own_late, early, late)


def per_device(sizes, tokens, norm_gain, gate_weight, up_weight, down_weight, slice_grads):
    move = lambda value, to: moved(value, sizes, to)
    y, x, k = lax.axis_index("y"), lax.axis_index("x"), lax.axis_index("k")
    packed = pack(norm_gain, gate_weight, up_weight, down_weight.T)
    near = lax.all_gather(packed, ("z", "k"), axis=0, tiled=True)
    near = jnp.concatenate(
        [
            lax.dynamic_slice(near, (0, k * WIDE), (SHARE, WIDE)),
            lax.dynamic_slice(near, (k * HALF, 2 * WIDE), (HALF, WIDE)),
        ]
    )
    near, grads = lax.optimization_barrier((near, slice_grads[0]))
    mine = grads.astype(jnp.bfloat16)
    line = {m: move(near, first_axis(m)) for m in (1, 3, 2)}
    line[0] = near
    far = move(mine, over_cuts(1))
    both_tokens = (tokens, move(tokens, other_core))

    own = {}
    for h in range(2):
        own[0, h] = jnp.stack([line[j] for j in HALVES[h]])
    own[1, 0] = move(own[0, 0], second_axis(1))
    own[3, 1] = move(own[0, 1], second_axis(3))
    own[1, 1] = move(own[0, 1], second_axis(1))
    own[3, 0] = move(own[0, 0], second_axis(3))
    own[2, 0] = move(own[1, 0], second_axis(3))
    own[2, 1] = move(own[3, 1], second_axis(1))

    a, j = jnp.arange(16) // 4, jnp.arange(16) % 4
    place = lambda core: (y ^ jnp.where(core == 0, a, j)) * 4 + (x ^ jnp.where(core == 0, j, a))
    at = jnp.concatenate(
        [
            place(k) * SHARE,
            place(k) * SHARE + k * HALF,
            place(1 - k) * SHARE + (1 - k) * HALF,
            k[None],
        ]
    ).astype(jnp.int32)

    total, own_early, late_tokens = early_sums(at, both_tokens, own)
    early = move(own_early, other_core)
    pair = (mine.astype(jnp.float32) + far.astype(jnp.float32)).astype(jnp.bfloat16)
    rest = move(pair, over_cuts(3))
    grad_mean = (pair.astype(jnp.float32) + rest.astype(jnp.float32)) / sizes[0]
    own_late = late_sums(total, late_tokens, tokens.shape[0], own)
    late = move(own_late, other_core)
    branch = down(at, own_early, own_late, early, late, tokens)
    return branch, grad_mean


def solution(mesh):
    cuts = mesh.shape["cuts"]
    sizes = (cuts, 4, 4, 4, 2)
    finer = Mesh(mesh.devices.reshape(sizes), AXES)
    in_specs = (
        P(AXES, None),
        P(FSDP),
        P(FSDP, None),
        P(FSDP, None),
        P(None, FSDP),
        P("c", None, FSDP, None),
    )
    out_specs = (P(AXES, None), P(None, FSDP, None))

    def body(*args):
        return per_device(sizes, *args)

    return jax.shard_map(
        body, mesh=finer, in_specs=in_specs, out_specs=out_specs, check_vma=False
    )
```

```python
import functools
import itertools

import jax
import jax.numpy as jnp
from jax import lax
from jax.experimental import pallas as pl
from jax.experimental.pallas import tpu as pltpu
from jax.sharding import Mesh
from jax.sharding import PartitionSpec as P

AXES = ("c", "y", "x", "z", "k")
FSDP = AXES[1:]
SUM_DIMS = (((1,), (0,)), ((), ()))
ROW_DIMS = (((1,), (1,)), ((), ()))
VMEM = pl.BlockSpec(memory_space=pltpu.VMEM)
SMEM = pl.BlockSpec(memory_space=pltpu.SMEM)
ANY = pl.BlockSpec(memory_space=pl.ANY)
HBM = pl.BlockSpec(memory_space=pltpu.HBM)
EPS = 1e-05
LANES = 128
SHARE, HALF, WIDE = 512, 256, 256
HALVES = ((0, 1), (3, 2))
EARLY = ((0, 0), (0, 1), (1, 0), (3, 1), (1, 1), (3, 0))
LATE = ((2, 1), (2, 0))
ORDER = EARLY + LATE


def moved(value, sizes, to):
    index = lambda at: functools.reduce(lambda i, s: i * s[1] + s[0], zip(at, sizes), 0)
    pairs = [(index(at), index(to(*at))) for at in itertools.product(*map(range, sizes))]
    return lax.ppermute(value, AXES, pairs)


def over_cuts(m):
    return lambda c, y, x, z, k: (c ^ m, y, x, z, k)


def other_core(c, y, x, z, k):
    return (c, y, x, z, 1 - k)


def first_axis(m):
    return lambda c, y, x, z, k: (c, y ^ (m * k), x ^ (m * (1 - k)), z, k)


def second_axis(m):
    return lambda c, y, x, z, k: (c, y ^ (m * (1 - k)), x ^ (m * k), z, k)


def pack_kernel(gain_hbm, gate_hbm, up_hbm, down_hbm, out_ref, gain_ref, gate_ref, up_ref, sems):
    f = gate_hbm.shape[1]
    copies = [
        pltpu.make_async_copy(a, b, sems.at[n])
        for n, (a, b) in enumerate(
            [
                (gain_hbm, gain_ref),
                (gate_hbm, gate_ref),
                (up_hbm, up_ref),
                (down_hbm, out_ref.at[:, 2 * f :]),
            ]
        )
    ]
    for copy in copies:
        copy.start()
    for copy in copies:
        copy.wait()
    rows = gate_hbm.shape[0]
    at = lambda d: lax.broadcasted_iota(jnp.int32, (rows, rows), d)
    gain = jnp.where(at(0) == at(1), gain_ref[...].astype(jnp.float32), 0.0)
    gain = jnp.sum(gain, axis=1, keepdims=True)
    gate = (gate_ref[...].astype(jnp.float32) * gain).astype(out_ref.dtype)
    up = (up_ref[...].astype(jnp.float32) * gain).astype(out_ref.dtype)
    h = f // 2
    for k in range(2):
        for n, w in enumerate((gate, up)):
            out_ref[:, (2 * k + n) * h : (2 * k + n + 1) * h] = w[:, k * h : (k + 1) * h]


def pack(gain, gate, up, down):
    rows, f = gate.shape
    return pl.pallas_call(
        pack_kernel,
        out_shape=jax.ShapeDtypeStruct((rows, 3 * f), gate.dtype),
        in_specs=[ANY] * 4,
        out_specs=VMEM,
        scratch_shapes=[
            pltpu.VMEM((1, rows), gate.dtype),
            pltpu.VMEM((rows, f), gate.dtype),
            pltpu.VMEM((rows, f), gate.dtype),
            pltpu.SemaphoreType.DMA((4,)),
        ],
        name="pack",
    )(gain[None, :], gate, up, down)


def token_copies(steps, at_ref, toks, tok_ref, sems):
    rows = toks[0].shape[0]
    copies = []
    for s, (a, half) in enumerate(steps):
        for i, j in enumerate(HALVES[half]):
            start = pl.multiple_of(at_ref[4 * a + j], SHARE)
            for who in range(2):
                copies.append(
                    pltpu.make_async_copy(
                        toks[who].at[:, pl.ds(start, SHARE)],
                        tok_ref.at[s, i, who * rows : (who + 1) * rows, :],
                        sems.at[s, i, who],
                    )
                )
    return copies


def add_piece(total, square, tok, gate_up):
    total += lax.dot_general(tok, gate_up, SUM_DIMS, preferred_element_type=jnp.float32)
    for l in range(0, SHARE, LANES):
        t = tok[:, l : l + LANES].astype(jnp.float32)
        square += t * t
    return total, square


def early_kernel(at_ref, *refs):
    n = len(EARLY)
    toks, pieces = refs[:2], list(refs[2 : 2 + n])
    out_ref, down_ref, late_tok_ref, tok_ref, held, sems, late_sems, held_sems = refs[2 + n :]
    loads = {}
    for i in range(held.shape[0]):
        s = n - held.shape[0] + i
        loads[s] = pltpu.make_async_copy(pieces[s], held.at[i], held_sems.at[i])
        pieces[s] = held.at[i]
    copies = token_copies(EARLY, at_ref, toks, tok_ref, sems)
    late_copies = token_copies(LATE, at_ref, toks, late_tok_ref, late_sems)
    for copy in copies[:8] + list(loads.values()) + copies[8:] + late_copies:
        copy.start()
    total = jnp.zeros((2 * toks[0].shape[0], WIDE), jnp.float32)
    square = jnp.zeros((2 * toks[0].shape[0], LANES), jnp.float32)
    for s in range(n):
        if s in loads:
            loads[s].wait()
        down_ref[s] = pieces[s][:, SHARE:, :]
        for i in range(2):
            for who in range(2):
                copies[4 * s + 2 * i + who].wait()
            total, square = add_piece(total, square, tok_ref[s, i], pieces[s][i, :SHARE, :])
    out_ref[:, :WIDE] = total
    out_ref[:, WIDE:] = square
    for copy in late_copies:
        copy.wait()


def late_kernel(before_ref, tok_ref, *refs):
    n = len(LATE)
    pieces, send_ref = refs[:n], refs[n]
    rows = tok_ref.shape[2] // 2
    for part, (s, i) in enumerate(itertools.product(range(n), range(2))):
        send_ref[part * HALF : (part + 1) * HALF, :] = pieces[s][i, SHARE:, :]
    total, square = before_ref[:, :WIDE], before_ref[:, WIDE:]
    for s, i in itertools.product(range(n), range(2)):
        total, square = add_piece(total, square, tok_ref[s, i], pieces[s][i, :SHARE, :])
    mean = jnp.sum(square, axis=1, keepdims=True) / (2 * len(ORDER) * SHARE)
    total = total * lax.rsqrt(mean + EPS)
    gate, up = total[:, : WIDE // 2], total[:, WIDE // 2 :]
    hidden = (gate / (1.0 + jnp.exp(-gate)) * up).astype(jnp.bfloat16)
    send_ref[2 * n * HALF :, : WIDE // 2] = hidden[rows:]
    send_ref[2 * n * HALF :, WIDE // 2 :] = hidden[:rows]


def sums_params(n):
    return dict(
        compiler_params=pltpu.CompilerParams(vmem_limit_bytes=8 * 2**20),
        cost_estimate=pl.CostEstimate(flops=n * 2**30, bytes_accessed=n * 2**20, transcendentals=0),
    )


def early_sums(at, tokens, pieces):
    n, m, rows = len(EARLY), len(LATE), tokens[0].shape[0]
    return pl.pallas_call(
        early_kernel,
        out_shape=[
            jax.ShapeDtypeStruct((2 * rows, WIDE + LANES), jnp.float32),
            jax.ShapeDtypeStruct((n, 2, HALF, WIDE), jnp.bfloat16),
            jax.ShapeDtypeStruct((m, 2, 2 * rows, SHARE), jnp.bfloat16),
        ],
        in_specs=[SMEM] + [HBM] * 2 + [VMEM] * (n - 2) + [HBM] * 2,
        out_specs=[VMEM, VMEM, VMEM],
        scratch_shapes=[
            pltpu.VMEM((n, 2, 2 * rows, SHARE), jnp.bfloat16),
            pltpu.VMEM((2, 2, SHARE + HALF, WIDE), jnp.bfloat16),
            pltpu.SemaphoreType.DMA((n, 2, 2)),
            pltpu.SemaphoreType.DMA((m, 2, 2)),
            pltpu.SemaphoreType.DMA((2,)),
        ],
        name="early",
        **sums_params(n),
    )(at, *tokens, *[pieces[s] for s in EARLY])


def late_sums(before, late_tokens, rows, pieces):
    n = len(LATE)
    return pl.pallas_call(
        late_kernel,
        out_shape=jax.ShapeDtypeStruct((2 * n * HALF + rows, WIDE), jnp.bfloat16),
        in_specs=[VMEM] * (2 + n),
        out_specs=VMEM,
        name="late",
        **sums_params(n),
    )(before, late_tokens, *[pieces[s] for s in LATE])


def down_kernel(at_ref, own_early_ref, own_late_ref, early_ref, late_ref, out_ref, held, sems):
    half = WIDE // 2
    hid = 2 * len(LATE) * HALF
    mine, theirs = own_late_ref[hid:, half:], late_ref[hid:, :half]
    hidden = jnp.where(
        at_ref[48] == 0,
        jnp.concatenate([mine, theirs], axis=1),
        jnp.concatenate([theirs, mine], axis=1),
    )

    def rows(who, a, j):
        half = 0 if j in HALVES[0] else 1
        s, i = ORDER.index((a, half)), HALVES[half].index(j)
        if s < len(EARLY):
            return (own_early_ref, early_ref)[who][s, i]
        part = 2 * (s - len(EARLY)) + i
        return (own_late_ref, late_ref)[who][part * HALF : (part + 1) * HALF, :]

    copies = []
    for slot, (a, j) in enumerate(itertools.product(range(4), range(4))):
        for who, block in enumerate((rows(0, a, j), rows(1, j, a))):
            out = lax.dot_general(hidden, block, ROW_DIMS, preferred_element_type=jnp.float32)
            side = at_ref[48] if who == 0 else 1 - at_ref[48]
            lanes = pl.ds(pl.multiple_of(side * HALF, HALF), HALF)
            held[slot, :, lanes] = out.astype(held.dtype)
        start = pl.multiple_of(at_ref[slot], SHARE)
        copy = pltpu.make_async_copy(held.at[slot], out_ref.at[:, pl.ds(start, SHARE)], sems.at[slot])
        copy.start()
        copies.append(copy)
    for copy in copies:
        copy.wait()


def down(at, own_early, own_late, early, late, tokens):
    n = len(ORDER)
    return pl.pallas_call(
        down_kernel,
        out_shape=jax.ShapeDtypeStruct(tokens.shape, jnp.bfloat16),
        in_specs=[SMEM] + [VMEM] * 4,
        out_specs=HBM,
        scratch_shapes=[
            pltpu.VMEM((2 * n, tokens.shape[0], SHARE), jnp.bfloat16),
            pltpu.SemaphoreType.DMA((2 * n,)),
        ],
        compiler_params=pltpu.CompilerParams(vmem_limit_bytes=8 * 2**20),
        name="down",
    )(at, own_early, own_late, early, late)


def per_device(sizes, tokens, norm_gain, gate_weight, up_weight, down_weight, slice_grads):
    move = lambda value, to: moved(value, sizes, to)
    y, x, k = lax.axis_index("y"), lax.axis_index("x"), lax.axis_index("k")
    packed = pack(norm_gain, gate_weight, up_weight, down_weight.T)
    near = lax.all_gather(packed, ("z", "k"), axis=0, tiled=True)
    near = jnp.concatenate(
        [
            lax.dynamic_slice(near, (0, k * WIDE), (SHARE, WIDE)),
            lax.dynamic_slice(near, (k * HALF, 2 * WIDE), (HALF, WIDE)),
        ]
    )
    near, grads = lax.optimization_barrier((near, slice_grads[0]))
    mine = grads.astype(jnp.bfloat16)
    line = {m: move(near, first_axis(m)) for m in (1, 3, 2)}
    line[0] = near
    far = move(mine, over_cuts(1))
    both_tokens = (tokens, move(tokens, other_core))

    own = {}
    for h in range(2):
        own[0, h] = jnp.stack([line[j] for j in HALVES[h]])
    own[1, 0] = move(own[0, 0], second_axis(1))
    own[3, 1] = move(own[0, 1], second_axis(3))
    own[1, 1] = move(own[0, 1], second_axis(1))
    own[3, 0] = move(own[0, 0], second_axis(3))
    own[2, 0] = move(own[1, 0], second_axis(3))
    own[2, 1] = move(own[3, 1], second_axis(1))

    a, j = jnp.arange(16) // 4, jnp.arange(16) % 4
    place = lambda core: (y ^ jnp.where(core == 0, a, j)) * 4 + (x ^ jnp.where(core == 0, j, a))
    at = jnp.concatenate(
        [
            place(k) * SHARE,
            place(k) * SHARE + k * HALF,
            place(1 - k) * SHARE + (1 - k) * HALF,
            k[None],
        ]
    ).astype(jnp.int32)

    total, own_early, late_tokens = early_sums(at, both_tokens, own)
    early = move(own_early, other_core)
    pair = (mine.astype(jnp.float32) + far.astype(jnp.float32)).astype(jnp.bfloat16)
    rest = move(pair, over_cuts(3))
    grad_mean = (pair.astype(jnp.float32) + rest.astype(jnp.float32)) / sizes[0]
    own_late = late_sums(total, late_tokens, tokens.shape[0], own)
    late = move(own_late, other_core)
    branch = down(at, own_early, own_late, early, late, tokens)
    return branch, grad_mean


def solution(mesh):
    cuts = mesh.shape["cuts"]
    sizes = (cuts, 4, 4, 4, 2)
    finer = Mesh(mesh.devices.reshape(sizes), AXES)
    in_specs = (
        P(AXES, None),
        P(FSDP),
        P(FSDP, None),
        P(FSDP, None),
        P(None, FSDP),
        P("c", None, FSDP, None),
    )
    out_specs = (P(AXES, None), P(None, FSDP, None))

    def body(*args):
        return per_device(sizes, *args)

    return jax.shard_map(
        body, mesh=finer, in_specs=in_specs, out_specs=out_specs, check_vma=False
    )
```
